32 devices in a mesh: pool: 2 (over x), pencil: 8 (over z, y), tgroup: 2 (over core).
Axes of the slice: x: 2, y: 2, z: 4, core: 2. Of those that a mesh axis runs over, the one named last changes fastest.
Arguments:
- dpsi: float32 [2, 4, 196608], P(None, 'pool', ('pencil', 'tgroup')), parts along dimension 1, may hold values from -6 to 6
- stick_cols: int32 [3072], replicated, may hold values from 0 to 16383, as said below
- pw_z: int32 [3072, 64], P('pencil'), may hold values from 0 to 127, as said below
- v_local: float32 [128, 16384], P('pencil'), may hold values from -6 to 6
- dv: float32 [128, 16384], P('pencil'), may hold values from -6 to 6
Outputs:
- h_dpsi: float32 [2, 4, 196608], P(None, 'pool', ('pencil', 'tgroup')), parts along dimension 1
The draws below stay inside these ranges and needn't reach their ends.
There are 2 independent parts, one for each index of `pool`. The reference program is written for one: setup_inputs(seed, part) draws one part's arguments, and reference() takes and returns one part's arrays. A program takes and returns all parts, laid end to end along the dimension named above; an argument that names none is the same for every part. Nothing has to cross between parts.
Inputs may be any that keep to these rules, and one draw needn't show every extreme that they name: `stick_cols`: the 3072 values are distinct. `pw_z`: the 64 values of each row are distinct.
All inputs are finite; a program needn't handle non-finite values.
Results may differ from the reference program's by a relative error of at most 0.00007.
Values sent between devices are 32-bit elements; how exact they have to be, the bound alone decides.
No kernel may reach another device: no remote copies, remote signals or barrier semaphores. Data moves between devices by JAX's collectives and lax.ppermute only.
A program may use at most 128 MiB of HBM per device.

```python
import jax
import jax.numpy as jnp
from jax import lax

N = 128
STICKS = 3072
ZPW = 64
BANDS = 2
NPW = 196608


def draw_stick_cols(key, part):
    column = jnp.arange(N * N, dtype=jnp.int32)
    first = column // N
    second = column % N
    freq_x = jnp.where(first < N // 2, first, first - N)
    freq_y = jnp.where(second < N // 2, second, second - N)
    radius = freq_x * freq_x + freq_y * freq_y
    breaker = jax.random.permutation(jax.random.fold_in(key, 11), N * N).astype(jnp.int32)
    scores = radius * (N * N) + breaker
    chosen = jnp.argsort(scores, stable=True)[:STICKS].astype(jnp.int32)
    return jax.random.permutation(jax.random.fold_in(key, 12), chosen).astype(jnp.int32)


def draw_pw_z(key, part):
    noise = jax.random.randint(jax.random.fold_in(key, 21), (STICKS, N), 0, 2 ** 20)
    scores = noise * N + jnp.arange(N, dtype=jnp.int32)[None, :]
    return jnp.argsort(scores, axis=1, stable=True)[:, :ZPW].astype(jnp.int32)


def steps_of(rng, extent, pieces, least, top_value):
    level = 1.0
    for dim, blocks in pieces:
        steps = jax.random.uniform(jax.random.fold_in(jax.random.fold_in(rng, 6), dim), (blocks,), jnp.float32, least / len(pieces), top_value / len(pieces))
        level = level * jnp.repeat(jnp.exp(steps), extent[dim] // blocks).reshape((-1,) + (1,) * (len(extent) - 1 - dim))
    return level


def bell_draw(own_key, dims, scale, bound, pieces=(), kind=jnp.bfloat16):
    entries = jax.random.normal(own_key, dims, jnp.float32) * scale
    if len(pieces) > 0:
        entries = steps_of(own_key, dims, pieces, -0.22, 0.18) * entries
    return jnp.clip(entries, min=-bound, max=bound).astype(kind)


def setup_inputs(seed: int = 0, part: int = 0) -> dict:
    seeds = jax.random.split(jax.random.key(seed), 6)
    part_keys = jax.random.split(jax.random.fold_in(seeds[5], part), 6)
    return {
        "dpsi": bell_draw(part_keys[0], (2, BANDS, NPW), 1.0, 6.0, ((2, 16),), jnp.float32),
        "stick_cols": draw_stick_cols(jax.random.fold_in(seeds[5], 71), part),
        "pw_z": draw_pw_z(jax.random.fold_in(seeds[5], 71), part),
        "v_local": bell_draw(seeds[3], (N, N * N), 1.0, 6.0, ((0, 8),), jnp.float32),
        "dv": bell_draw(seeds[4], (N, N * N), 0.5, 6.0, ((0, 8),), jnp.float32),
    }


def reference(dpsi, stick_cols, pw_z, v_local, dv):
    potential = (v_local + dv).reshape(N, N, N).transpose(1, 2, 0)
    scale = float(N) ** 1.5
    rows = stick_cols[:, None].astype(jnp.int32)
    depth = pw_z.astype(jnp.int32)

    def one_band(band):
        coeffs = (band[0] + 1j * band[1]).reshape(STICKS, ZPW)
        grid = jnp.zeros((N * N, N), coeffs.dtype).at[rows, depth].set(coeffs)
        wave = jnp.fft.ifftn(grid.reshape(N, N, N)) * scale
        result = jnp.fft.fftn(potential * wave) / scale
        picked = result.reshape(N * N, N)[rows, depth].reshape(NPW)
        return jnp.stack([jnp.real(picked), jnp.imag(picked)])

    output = lax.map(one_band, dpsi.transpose(1, 0, 2))
    return output.transpose(1, 0, 2)
```

```python
import math

import jax
import jax.numpy as jnp
import numpy as np
from jax import lax
from jax.experimental import pallas as pl
from jax.experimental.pallas import tpu as pltpu
from jax.sharding import PartitionSpec as P

N = 128
LANES = 128
SUB = 8


def transform_matrix():
    phase = np.outer(np.arange(N), np.arange(N)) % N
    angle = phase.astype(np.float64) * (2.0 * math.pi / N)
    re = np.cos(angle) / math.sqrt(N)
    im = np.sin(angle) / math.sqrt(N)
    return np.block([[re, im], [-im, re]])


def split_table(table):
    table = jnp.asarray(table, jnp.float32)
    high = table.astype(jnp.bfloat16)
    low = (table - high.astype(jnp.float32)).astype(jnp.bfloat16)
    return high, low


def const_split(table):
    bf = jnp.bfloat16
    t32 = np.asarray(table, np.float32)
    high = t32.astype(bf)
    low = (t32 - high.astype(np.float32)).astype(bf)
    return jnp.asarray(high), jnp.asarray(low)


def split(value):
    high = value.astype(jnp.bfloat16)
    low = (value - high.astype(jnp.float32)).astype(jnp.bfloat16)
    return high, low


def dot(a, b, dims):
    return lax.dot_general(a, b, (dims, ((), ())), preferred_element_type=jnp.float32)


def lane_gather(values, index):
    return jnp.take_along_axis(values, index, axis=1, mode="promise_in_bounds")


def stick_index_kernel(zpw):
    def body(pw_ref, inv_ref, twice_ref):
        sticks = inv_ref.shape[0]
        step = 2 * SUB

        def tile(i, carry):
            spread = lax.broadcasted_iota(jnp.int32, (step, N), 1)
            at = pl.ds(pl.multiple_of(i * step, step), step)
            pw = pw_ref[at, :]
            acc = jnp.full((step, N), -1, jnp.int32)
            for k in range(zpw):
                acc = jnp.where(pw[:, k : k + 1] == spread, k, acc)
            inv_ref[at, :] = acc
            twice_ref[at, :] = jnp.concatenate([pw, pw], axis=1)
            return carry

        lax.fori_loop(0, sticks // step, tile, 0)

    return body


def column_index_kernel(blocks, per_block):
    def body(cols_ref, chunk_ref, lane_ref):
        me = lax.axis_index("pencil")
        row = lax.broadcasted_iota(jnp.int32, (N, LANES), 0)
        lane = lax.broadcasted_iota(jnp.int32, (N, LANES), 1).astype(jnp.float32)
        chunk_sum = jnp.zeros((N, N), jnp.float32)
        lane_sum = jnp.zeros((N, N), jnp.float32)
        nt = ((1,), (1,))
        for g in range(blocks * per_block):
            cols = cols_ref[g : g + 1, :]
            place = ((me ^ (g // per_block)) * per_block + g % per_block + 1).astype(jnp.float32)
            at_x = (cols >> 7) == row
            at_y = jnp.where((cols & (N - 1)) == row, 1.0, 0.0).astype(jnp.bfloat16)
            chunk_sum += dot(jnp.where(at_x, place, 0.0).astype(jnp.bfloat16), at_y, nt)
            lane_sum += dot(jnp.where(at_x, lane, 0.0).astype(jnp.bfloat16), at_y, nt)
        chunk_ref[...] = chunk_sum.astype(jnp.int32) - 1
        lane_ref[...] = lane_sum.astype(jnp.int32)

    return body


def up_kernel(blocks, rows, zpw):
    def body(own_ref, other_ref, inv_ref, high_ref, low_ref, *rest):
        outs = rest[:blocks]
        grid_ref, field_ref = rest[blocks:]
        me = lax.axis_index("pencil")
        first = lax.axis_index("tgroup") == 0
        pairs = inv_ref.shape[0] // 2
        half = pairs // 2
        for part in range(2):
            own = jnp.where(
                first,
                own_ref[part, pl.ds(0, half, stride=2), :],
                own_ref[part, pl.ds(1, half, stride=2), :],
            )
            other = other_ref[part]
            coeff = jnp.concatenate([jnp.where(first, own, other), jnp.where(first, other, own)], axis=0)
            for parity in range(2):
                index = inv_ref[pl.ds(parity, pairs, stride=2), :]
                value = lane_gather(coeff, jnp.maximum(index, 0) + parity * zpw)
                grid_ref[part, pl.ds(parity, pairs, stride=2), :] = jnp.where(index >= 0, value, 0.0)
        high, low = split(jnp.concatenate([grid_ref[0], grid_ref[1]], axis=1))
        left = jnp.concatenate([high_ref[...], low_ref[...], high_ref[...]], axis=1)
        right = jnp.concatenate([high, high, low], axis=1)
        field_ref[...] = dot(left, right, ((1,), (1,)))
        for d in range(blocks):
            outs[d][...] = field_ref[pl.ds(pl.multiple_of((me ^ d) * rows, SUB), rows), :]

    return body


def quarter_swap(value):
    top = jnp.concatenate([value[:N, :N], value[N:, :N]], axis=1)
    bottom = jnp.concatenate([value[:N, N:], value[N:, N:]], axis=1)
    return jnp.concatenate([top, bottom], axis=0)


def plane_kernel(blocks, per_block, width, planes):
    chunks = blocks * per_block
    slots = -(-chunks // SUB) * SUB
    plane_rows = min(planes, SUB)
    tiles = N // SUB

    def body(*refs):
        fields = refs[:blocks]
        chunk_ref, lane_ref, cols_ref, v_ref, dv_ref, mh_ref, ml_ref, th_ref, tl_ref = refs[blocks : blocks + 9]
        outs = refs[blocks + 9 : 2 * blocks + 9]
        in_ref, grid_ref, out_ref = refs[2 * blocks + 9 :]
        me = lax.axis_index("pencil")
        rows = 2 * planes
        for d in range(blocks):
            for k in range(per_block):
                w = min(LANES, width - k * LANES)
                in_ref[pl.ds(d * per_block + k, rows, stride=slots), :w] = fields[d][:, k * LANES : k * LANES + w]

        def pair(pp, carry):
            def fill(xt, c):
                at = pl.multiple_of(xt * SUB, SUB)
                lane = lane_ref[pl.ds(at, SUB), :]
                chunk = chunk_ref[pl.ds(at, SUB), :]
                for part in range(2):
                    for h in range(2):
                        base = pl.multiple_of((part * planes + pp * 2 + h) * slots, SUB)
                        acc = jnp.zeros((SUB, N), jnp.float32)
                        for g in range(chunks):
                            source = jnp.broadcast_to(in_ref[pl.ds(base + g, 1), :], (SUB, LANES))
                            acc = jnp.where(chunk == g, lane_gather(source, lane), acc)
                        grid_ref[pl.ds(pl.multiple_of(h * N + at, SUB), SUB), part * N : (part + 1) * N] = acc
                return c

            lax.fori_loop(0, tiles, fill, 0)

            def right_apply(value, high_ref, low_ref):
                high, low = split(value)
                left = jnp.concatenate([high, low, high], axis=1)
                right = jnp.concatenate([high_ref[...], high_ref[...], low_ref[...]], axis=0)
                return dot(left, right, ((1,), (0,)))

            def left_apply(value, high_ref, low_ref):
                high, low = split(value)
                left = jnp.concatenate([high_ref[...], low_ref[...], high_ref[...]], axis=1)
                right = jnp.concatenate([high, high, low], axis=0)
                return dot(left, right, ((1,), (0,)))

            along = right_apply(grid_ref[...], mh_ref, ml_ref)
            space = left_apply(quarter_swap(along), th_ref, tl_ref)
            weights = []
            for h in range(2):
                plane = pp * 2 + h
                at = (plane // plane_rows) * (plane_rows * N) + plane % plane_rows
                weights.append(v_ref[pl.ds(at, N, stride=plane_rows), :] + dv_ref[pl.ds(at, N, stride=plane_rows), :])
            weight = jnp.concatenate(weights, axis=1)
            space = space * jnp.concatenate([weight, weight], axis=0)
            back = left_apply(space, mh_ref, ml_ref)
            grid_ref[...] = right_apply(quarter_swap(back), th_ref, tl_ref)

            def pick(g, c):
                source_chunk = (me ^ (g // per_block)) * per_block + g % per_block
                cols = jnp.broadcast_to(cols_ref[pl.ds(source_chunk, 1), :], (SUB, LANES))
                at_x = cols >> 7
                at_y = cols & (N - 1)
                sub = lax.broadcasted_iota(jnp.int32, (SUB, LANES), 0)
                for part in range(2):
                    for h in range(2):
                        acc = jnp.zeros((SUB, LANES), jnp.float32)
                        for xt in range(tiles):
                            source = grid_ref[h * N + xt * SUB : h * N + (xt + 1) * SUB, part * N : (part + 1) * N]
                            acc = jnp.where(at_x == sub + xt * SUB, lane_gather(source, at_y), acc)
                        total = jnp.sum(acc, axis=0, keepdims=True)
                        out_ref[pl.ds((part * planes + pp * 2 + h) * slots + g, 1), :] = total
                return c

            lax.fori_loop(0, chunks, pick, 0)
            return carry

        lax.fori_loop(0, planes // 2, pair, 0)
        for d in range(blocks):
            for k in range(per_block):
                w = min(LANES, width - k * LANES)
                outs[d][:, k * LANES : k * LANES + w] = out_ref[pl.ds(d * per_block + k, rows, stride=slots), :w]

    return body


def down_kernel(blocks, rows, zpw):
    def body(*refs):
        fields = refs[:blocks]
        pw_ref, high_ref, low_ref, own_ref, other_ref, field_ref, grid_ref = refs[blocks:]
        me = lax.axis_index("pencil")
        first = lax.axis_index("tgroup") == 0
        for d in range(blocks):
            field_ref[pl.ds(pl.multiple_of((me ^ d) * rows, SUB), rows), :] = fields[d][...]
        high, low = split(field_ref[...])
        left = jnp.concatenate([high, low, high], axis=0)
        right = jnp.concatenate([high_ref[...], high_ref[...], low_ref[...]], axis=0)
        grid = dot(left, right, ((0,), (0,)))
        pairs = grid.shape[0] // 2
        half = pairs // 2
        even = pl.ds(0, pairs, stride=2)
        odd = pl.ds(1, pairs, stride=2)
        lane = lax.broadcasted_iota(jnp.int32, (pairs, LANES), 1)
        index = jnp.where(lane < zpw, pw_ref[even, :], pw_ref[odd, :])
        for part in range(2):
            grid_ref[part] = grid[:, part * N : (part + 1) * N]
            a = lane_gather(grid_ref[part, even, :], index)
            b = lane_gather(grid_ref[part, odd, :], index)
            picked = jnp.where(lane < zpw, a, b)
            own_ref[part] = jnp.where(first, picked[:half], picked[half:])
            other_ref[part] = jnp.where(first, picked[half:], picked[:half])

    return body


def call(body, outs, scratch, args):
    vmem = pl.BlockSpec(memory_space=pltpu.VMEM)
    many = isinstance(outs, (list, tuple))
    return pl.pallas_call(
        body,
        out_shape=outs,
        in_specs=[vmem] * len(args),
        out_specs=[vmem] * len(outs) if many else vmem,
        scratch_shapes=scratch,
    )(*args)


def local(dpsi, stick_cols, pw_z, v_local, dv):
    blocks = lax.axis_size("pencil")
    bands = dpsi.shape[1]
    sticks, zpw = pw_z.shape
    planes = v_local.shape[0]
    rows = 2 * planes
    pairs = sticks // 2
    half = pairs // 2
    per_block = -(-sticks // LANES)
    slots = -(-blocks * per_block // SUB) * SUB
    f32 = jnp.float32
    first = lax.axis_index("tgroup") == 0

    matrix = transform_matrix()
    mh, ml = const_split(matrix)
    th, tl = const_split(matrix.T)
    order = np.arange(2 * N).reshape(2, blocks, planes).transpose(1, 0, 2).reshape(-1)
    uh, ul = const_split(matrix.T[order])
    dh, dl = const_split(matrix.T[order])

    send = jnp.where(first, dpsi[:, 1], dpsi[:, 0]).reshape(2, half, LANES)
    swap = [(0, 1), (1, 0)]
    other = lax.ppermute(send, "tgroup", swap)
    own = dpsi.reshape(2, bands, half, LANES).transpose(0, 2, 1, 3).reshape(2, half * bands, LANES)

    lookup = jax.ShapeDtypeStruct((sticks, N), jnp.int32)
    inv, twice = call(stick_index_kernel(zpw), (lookup, lookup), [], (pw_z,))
    width = min(LANES, sticks)
    cols = stick_cols.reshape(blocks * per_block, width)
    if width < LANES:
        cols = jnp.pad(cols, ((0, 0), (0, LANES - width)), constant_values=-1)
    table = jax.ShapeDtypeStruct((N, N), jnp.int32)
    chunk, lane = call(column_index_kernel(blocks, per_block), (table, table), [], (cols,))

    block = jax.ShapeDtypeStruct((rows, sticks), f32)
    fields = call(
        up_kernel(blocks, rows, zpw),
        [block] * blocks,
        [pltpu.VMEM((2, sticks, N), f32), pltpu.VMEM((2 * N, sticks), f32)],
        (own, other, inv, uh, ul),
    )

    def exchange(parts):
        got = [parts[0]]
        for d in range(1, blocks):
            got.append(lax.ppermute(parts[d], "pencil", [(i, i ^ d) for i in range(blocks)]))
        return got

    plane_rows = min(planes, SUB)

    def by_column(values):
        return (
            values.reshape(planes // plane_rows, plane_rows, N, N)
            .transpose(0, 2, 1, 3)
            .reshape(planes * N, N)
        )

    applied = call(
        plane_kernel(blocks, per_block, sticks, planes),
        [block] * blocks,
        [
            pltpu.VMEM((rows * slots, LANES), f32),
            pltpu.VMEM((2 * N, 2 * N), f32),
            pltpu.VMEM((rows * slots, LANES), f32),
        ],
        (*exchange(fields), chunk, lane, cols, by_column(v_local), by_column(dv), mh, ml, th, tl),
    )
    side = jax.ShapeDtypeStruct((2, half, LANES), f32)
    mine, theirs = call(
        down_kernel(blocks, rows, zpw),
        [side, side],
        [pltpu.VMEM((2 * N, sticks), f32), pltpu.VMEM((2, sticks, N), f32)],
        (*exchange(applied), twice, dh, dl),
    )
    back = lax.ppermute(theirs, "tgroup", swap)
    mine = mine.reshape(2, 1, half * LANES)
    back = back.reshape(2, 1, half * LANES)
    return jnp.concatenate([jnp.where(first, mine, back), jnp.where(first, back, mine)], axis=1)


def solution(mesh):
    in_specs = (
        P(None, "pool", ("pencil", "tgroup")),
        P(),
        P("pencil", None),
        P("pencil", None),
        P("pencil", None),
    )
    out_specs = P(None, "pool", ("pencil", "tgroup"))
    return jax.shard_map(local, mesh=mesh, in_specs=in_specs, out_specs=out_specs, check_vma=False)
```

```python
import math

import jax
import jax.numpy as jnp
import numpy as np
from jax import lax
from jax.experimental import pallas as pl
from jax.experimental.pallas import tpu as pltpu
from jax.sharding import PartitionSpec as P

N = 128
LANES = 128
SUB = 8


def transform_matrix():
    phase = np.outer(np.arange(N), np.arange(N)) % N
    angle = phase.astype(np.float64) * (2.0 * math.pi / N)
    re = np.cos(angle) / math.sqrt(N)
    im = np.sin(angle) / math.sqrt(N)
    return np.block([[re, im], [-im, re]])


def const_split(table):
    bf = jnp.bfloat16
    t32 = np.asarray(table, np.float32)
    high = t32.astype(bf)
    low = (t32 - high.astype(np.float32)).astype(bf)
    return jnp.asarray(high), jnp.asarray(low)


def split(value):
    high = value.astype(jnp.bfloat16)
    low = (value - high.astype(jnp.float32)).astype(jnp.bfloat16)
    return high, low


def dot(a, b, dims):
    return lax.dot_general(a, b, (dims, ((), ())), preferred_element_type=jnp.float32)


def lane_gather(values, index):
    return jnp.take_along_axis(values, index, axis=1, mode="promise_in_bounds")


def stick_index_kernel(zpw):
    def body(pw_ref, inv_ref, twice_ref):
        sticks = inv_ref.shape[0]
        for at in range(0, sticks, LANES):
            w = min(LANES, sticks - at)
            pw = pw_ref[:, at : at + w]
            spread = lax.broadcasted_iota(jnp.int32, (N, w), 0)
            acc = jnp.full((N, w), -1, jnp.int32)
            for k in range(zpw):
                acc = jnp.where(pw[k : k + 1, :] == spread, k, acc)
            inv_ref[at : at + w, :] = acc.T
            twice_ref[at : at + w, :] = jnp.concatenate([pw, pw], axis=0).T

    return body


def up_kernel(blocks, rows, zpw):
    def body(own_ref, other_ref, inv_ref, high_ref, low_ref, *rest):
        outs = rest[:blocks]
        grid_ref, field_ref = rest[blocks:]
        me = lax.axis_index("pencil")
        first = lax.axis_index("tgroup") == 0
        pairs = inv_ref.shape[0] // 2
        half = pairs // 2
        for part in range(2):
            own = jnp.where(
                first,
                own_ref[part, pl.ds(0, half, stride=2), :],
                own_ref[part, pl.ds(1, half, stride=2), :],
            )
            other = other_ref[part]
            coeff = jnp.concatenate([jnp.where(first, own, other), jnp.where(first, other, own)], axis=0)
            for parity in range(2):
                index = inv_ref[pl.ds(parity, pairs, stride=2), :]
                value = lane_gather(coeff, jnp.maximum(index, 0) + parity * zpw)
                grid_ref[part, pl.ds(parity, pairs, stride=2), :] = jnp.where(index >= 0, value, 0.0)
        high, low = split(jnp.concatenate([grid_ref[0], grid_ref[1]], axis=1))
        left = jnp.concatenate([high_ref[...], low_ref[...], high_ref[...]], axis=1)
        right = jnp.concatenate([high, high, low], axis=1)
        field_ref[...] = dot(left, right, ((1,), (1,)))
        for d in range(blocks):
            outs[d][...] = field_ref[pl.ds(pl.multiple_of((me ^ d) * rows, SUB), rows), :]

    return body


def quarter_swap(value):
    top = jnp.concatenate([value[:N, :N], value[N:, :N]], axis=1)
    bottom = jnp.concatenate([value[:N, N:], value[N:, N:]], axis=1)
    return jnp.concatenate([top, bottom], axis=0)


def strides(planes):
    gap = SUB if planes % SUB == 0 else 0
    return planes + gap, 2 * planes + gap


def plane_kernel(blocks, per_block, sticks, planes):
    rows = 2 * planes
    fold = LANES // rows
    reach = N * N // fold
    reach_bits = reach.bit_length() - 1
    span = N // fold
    slots = per_block * LANES
    plane_rows = min(planes, SUB)
    along_stride, back_stride = strides(planes)
    unroll = 32

    def body(*refs):
        fields = refs[:blocks]
        smem_ref, cols_ref, v_ref, dv_ref, mh_ref, ml_ref, th_ref, tl_ref = refs[blocks : blocks + 8]
        outs = refs[blocks + 8 : 2 * blocks + 8]
        stick_ref, grid_ref, re_ref, im_ref, back_ref = refs[2 * blocks + 8 :]
        me = lax.axis_index("pencil")

        def right_apply(value, high_ref, low_ref):
            high, low = split(value)
            left = jnp.concatenate([high, low, high], axis=1)
            right = jnp.concatenate([high_ref[...], high_ref[...], low_ref[...]], axis=0)
            return dot(left, right, ((1,), (0,)))

        def left_apply(value, high_ref, low_ref):
            high, low = split(value)
            left = jnp.concatenate([high_ref[...], low_ref[...], high_ref[...]], axis=1)
            right = jnp.concatenate([high, high, low], axis=0)
            return dot(left, right, ((1,), (0,)))

        def each_stick(work):
            def block(q, c):
                def group(i, c2):
                    for j in range(unroll):
                        col = smem_ref[q * sticks + i * unroll + j]
                        work(q * slots + i * unroll + j, col & (reach - 1), col >> reach_bits)
                    return c2

                return lax.fori_loop(0, sticks // unroll, group, c)

            lax.fori_loop(0, blocks, block, 0)

        grid_ref[...] = jnp.zeros(grid_ref.shape, jnp.float32)
        for d in range(blocks):
            base = pl.multiple_of((me ^ d) * slots, LANES)
            for k in range(per_block):
                w = min(LANES, sticks - k * LANES)
                part = fields[d][:, k * LANES : k * LANES + w]
                stick_ref[pl.ds(base + k * LANES, w), :] = jnp.concatenate([part] * fold, axis=0).T

        quarter = lax.broadcasted_iota(jnp.int32, (1, LANES), 1) // rows

        def scatter(stick, place, sub):
            pltpu.store(grid_ref.at[pl.ds(place, 1), :], stick_ref[pl.ds(stick, 1), :], mask=quarter == sub)

        each_stick(scatter)

        step = 2 * N // planes

        def along(i, c):
            pieces = []
            for t in range(step // fold):
                at = pl.multiple_of((i * (step // fold) + t) * N, N)
                tile = grid_ref[pl.ds(at, N), :].T
                for u in range(fold):
                    lo = u * rows
                    pieces.append(jnp.concatenate([tile[lo : lo + planes], tile[lo + planes : lo + rows]], axis=1))
            value = right_apply(jnp.concatenate(pieces, axis=0), mh_ref, ml_ref)
            for x in range(step):
                at = ((x % fold) * span + i * (step // fold) + x // fold) * along_stride
                at = pl.multiple_of(at, SUB) if along_stride % SUB == 0 else at
                re_ref[pl.ds(at, planes), :] = value[x * planes : (x + 1) * planes, :N]
                im_ref[pl.ds(at, planes), :] = value[x * planes : (x + 1) * planes, N:]
            return c

        lax.fori_loop(0, N // step, along, 0)

        def pair(pp):
            tops, bottoms, weights = [], [], []
            for h in range(2):
                plane = pp * 2 + h
                pick = pl.ds(plane, N, stride=along_stride)
                tops.append(re_ref[pick, :])
                bottoms.append(im_ref[pick, :])
                at = pl.ds((plane // plane_rows) * (plane_rows * N) + plane % plane_rows, N, stride=plane_rows)
                weights.append(v_ref[at, :] + dv_ref[at, :])
            field = jnp.concatenate([jnp.concatenate(tops, axis=1), jnp.concatenate(bottoms, axis=1)], axis=0)
            space = left_apply(field, th_ref, tl_ref)
            weight = jnp.concatenate(weights, axis=1)
            space = space * jnp.concatenate([weight, weight], axis=0)
            back = left_apply(space, mh_ref, ml_ref)
            last = right_apply(quarter_swap(back), th_ref, tl_ref)
            for h in range(2):
                for part in range(2):
                    at = pl.ds(part * planes + pp * 2 + h, N, stride=back_stride)
                    back_ref[at, :] = last[h * N : (h + 1) * N, part * N : (part + 1) * N]

        def pairs(i, c):
            for j in range(2):
                pair(i * 2 + j)
            return c

        lax.fori_loop(0, planes // 4, pairs, 0)

        def turn(i, c):
            pieces = []
            for u in range(fold):
                at = (u * span + i) * back_stride
                pieces.append(back_ref[pl.ds(pl.multiple_of(at, SUB), rows), :])
            grid_ref[pl.ds(pl.multiple_of(i * N, N), N), :] = jnp.concatenate(pieces, axis=0).T
            return c

        lax.fori_loop(0, span, turn, 0)

        def fetch(stick, place, sub):
            stick_ref[pl.ds(stick, 1), :] = grid_ref[pl.ds(place, 1), :]

        each_stick(fetch)

        for d in range(blocks):
            for k in range(per_block):
                w = min(LANES, sticks - k * LANES)
                at = (me ^ d) * per_block + k
                tile = stick_ref[pl.ds(pl.multiple_of(at * LANES, LANES), LANES), :].T
                sub = cols_ref[pl.ds(at, 1), :] >> reach_bits
                value = tile[:rows]
                for u in range(1, fold):
                    value = jnp.where(sub == u, tile[u * rows : (u + 1) * rows], value)
                outs[d][:, k * LANES : k * LANES + w] = value[:, :w]

    return body


def down_kernel(blocks, rows, zpw):
    def body(*refs):
        fields = refs[:blocks]
        pw_ref, high_ref, low_ref, own_ref, other_ref, field_ref, grid_ref = refs[blocks:]
        me = lax.axis_index("pencil")
        first = lax.axis_index("tgroup") == 0
        for d in range(blocks):
            field_ref[pl.ds(pl.multiple_of((me ^ d) * rows, SUB), rows), :] = fields[d][...]
        high, low = split(field_ref[...])
        left = jnp.concatenate([high, low, high], axis=0)
        right = jnp.concatenate([high_ref[...], high_ref[...], low_ref[...]], axis=0)
        grid = dot(left, right, ((0,), (0,)))
        pairs = grid.shape[0] // 2
        half = pairs // 2
        even = pl.ds(0, pairs, stride=2)
        odd = pl.ds(1, pairs, stride=2)
        lane = lax.broadcasted_iota(jnp.int32, (pairs, LANES), 1)
        index = jnp.where(lane < zpw, pw_ref[even, :], pw_ref[odd, :])
        for part in range(2):
            grid_ref[part] = grid[:, part * N : (part + 1) * N]
            a = lane_gather(grid_ref[part, even, :], index)
            b = lane_gather(grid_ref[part, odd, :], index)
            picked = jnp.where(lane < zpw, a, b)
            own_ref[part] = jnp.where(first, picked[:half], picked[half:])
            other_ref[part] = jnp.where(first, picked[half:], picked[:half])

    return body


def call(body, outs, scratch, args, smem=()):
    vmem = pl.BlockSpec(memory_space=pltpu.VMEM)
    scalar = pl.BlockSpec(memory_space=pltpu.SMEM)
    many = isinstance(outs, (list, tuple))
    return pl.pallas_call(
        body,
        out_shape=outs,
        in_specs=[scalar if i in smem else vmem for i in range(len(args))],
        out_specs=[vmem] * len(outs) if many else vmem,
        scratch_shapes=scratch,
    )(*args)


def local(dpsi, stick_cols, pw_z, v_local, dv):
    blocks = lax.axis_size("pencil")
    bands = dpsi.shape[1]
    sticks, zpw = pw_z.shape
    planes = v_local.shape[0]
    rows = 2 * planes
    pairs = sticks // 2
    half = pairs // 2
    per_block = -(-sticks // LANES)
    f32 = jnp.float32
    first = lax.axis_index("tgroup") == 0

    matrix = transform_matrix()
    mh, ml = const_split(matrix)
    th, tl = const_split(matrix.T)
    order = np.arange(2 * N).reshape(2, blocks, planes).transpose(1, 0, 2).reshape(-1)
    uh, ul = const_split(matrix.T[order])
    dh, dl = const_split(matrix.T[order])

    send = jnp.where(first, dpsi[:, 1], dpsi[:, 0]).reshape(2, half, LANES)
    swap = [(0, 1), (1, 0)]
    other = lax.ppermute(send, "tgroup", swap)
    own = dpsi.reshape(2, bands, half, LANES).transpose(0, 2, 1, 3).reshape(2, half * bands, LANES)

    lookup = jax.ShapeDtypeStruct((sticks, N), jnp.int32)
    inv, twice = call(stick_index_kernel(zpw), (lookup, lookup), [], (pw_z.T,))
    width = min(LANES, sticks)
    cols = stick_cols.reshape(blocks * per_block, width)
    if width < LANES:
        cols = jnp.pad(cols, ((0, 0), (0, LANES - width)), constant_values=-1)
    block = jax.ShapeDtypeStruct((rows, sticks), f32)
    fields = call(
        up_kernel(blocks, rows, zpw),
        [block] * blocks,
        [pltpu.VMEM((2, sticks, N), f32), pltpu.VMEM((2 * N, sticks), f32)],
        (own, other, inv, uh, ul),
    )

    def exchange(parts):
        got = [parts[0]]
        for d in range(1, blocks):
            got.append(lax.ppermute(parts[d], "pencil", [(i, i ^ d) for i in range(blocks)]))
        return got

    plane_rows = min(planes, SUB)

    def by_column(values):
        return (
            values.reshape(planes // plane_rows, plane_rows, N, N)
            .transpose(0, 2, 1, 3)
            .reshape(planes * N, N)
        )

    fold = LANES // rows
    along_stride, back_stride = strides(planes)
    applied = call(
        plane_kernel(blocks, per_block, sticks, planes),
        [block] * blocks,
        [
            pltpu.VMEM((blocks * per_block * LANES, LANES), f32),
            pltpu.VMEM((N // fold * N, LANES), f32),
            pltpu.VMEM((N * along_stride, N), f32),
            pltpu.VMEM((N * along_stride, N), f32),
            pltpu.VMEM((N * back_stride, N), f32),
        ],
        (*exchange(fields), stick_cols, cols, by_column(v_local), by_column(dv), mh, ml, th, tl),
        smem=(blocks,),
    )
    side = jax.ShapeDtypeStruct((2, half, LANES), f32)
    mine, theirs = call(
        down_kernel(blocks, rows, zpw),
        [side, side],
        [pltpu.VMEM((2 * N, sticks), f32), pltpu.VMEM((2, sticks, N), f32)],
        (*exchange(applied), twice, dh, dl),
    )
    back = lax.ppermute(theirs, "tgroup", swap)
    mine = mine.reshape(2, 1, half * LANES)
    back = back.reshape(2, 1, half * LANES)
    return jnp.concatenate([jnp.where(first, mine, back), jnp.where(first, back, mine)], axis=1)


def solution(mesh):
    in_specs = (
        P(None, "pool", ("pencil", "tgroup")),
        P(),
        P("pencil", None),
        P("pencil", None),
        P("pencil", None),
    )
    out_specs = P(None, "pool", ("pencil", "tgroup"))
    return jax.shard_map(local, mesh=mesh, in_specs=in_specs, out_specs=out_specs, check_vma=False)
```

```python
import math

import jax
import jax.numpy as jnp
import numpy as np
from jax import lax
from jax.experimental import pallas as pl
from jax.experimental.pallas import tpu as pltpu
from jax.sharding import PartitionSpec as P

N = 128
LANES = 128
SUB = 8
UNROLL = 32


def transform_matrix():
    phase = np.outer(np.arange(N), np.arange(N)) % N
    angle = phase.astype(np.float64) * (2.0 * math.pi / N)
    re = np.cos(angle) / math.sqrt(N)
    im = np.sin(angle) / math.sqrt(N)
    return np.block([[re, im], [-im, re]])


def const_split(table):
    bf = jnp.bfloat16
    t32 = np.asarray(table, np.float32)
    high = t32.astype(bf)
    low = (t32 - high.astype(np.float32)).astype(bf)
    return jnp.asarray(high), jnp.asarray(low)


def split(value):
    high = value.astype(jnp.bfloat16)
    low = (value - high.astype(jnp.float32)).astype(jnp.bfloat16)
    return high, low


def dot(a, b, dims):
    return lax.dot_general(a, b, (dims, ((), ())), preferred_element_type=jnp.float32)


def lane_gather(values, index):
    return jnp.take_along_axis(values, index, axis=1, mode="promise_in_bounds")


def stick_index_kernel(zpw):
    def body(pw_ref, inv_ref, twice_ref):
        sticks = inv_ref.shape[0]
        for at in range(0, sticks, LANES):
            w = min(LANES, sticks - at)
            pw = pw_ref[:, at : at + w]
            spread = lax.broadcasted_iota(jnp.int32, (N, w), 0)
            acc = jnp.full((N, w), -1, jnp.int32)
            for k in range(zpw):
                acc = jnp.where(pw[k : k + 1, :] == spread, k, acc)
            inv_ref[at : at + w, :] = acc.T
            twice_ref[at : at + w, :] = jnp.concatenate([pw, pw], axis=0).T

    return body


def up_kernel(blocks, rows, zpw):
    def body(own_ref, other_ref, inv_ref, high_ref, low_ref, *rest):
        outs = rest[:blocks]
        grid_ref, field_ref = rest[blocks:]
        me = lax.axis_index("pencil")
        first = lax.axis_index("tgroup") == 0
        pairs = inv_ref.shape[0] // 2
        half = pairs // 2
        def mine(ref, part):
            low = ref[part, pl.ds(0, half, stride=2), :]
            high = ref[part, pl.ds(1, half, stride=2), :]
            return jnp.where(first, low, high)

        for part in range(2):
            own = mine(own_ref, part)
            other = mine(other_ref, part)
            coeff = jnp.concatenate([jnp.where(first, own, other), jnp.where(first, other, own)], axis=0)
            for parity in range(2):
                index = inv_ref[pl.ds(parity, pairs, stride=2), :]
                value = lane_gather(coeff, jnp.maximum(index, 0) + parity * zpw)
                grid_ref[part, pl.ds(parity, pairs, stride=2), :] = jnp.where(index >= 0, value, 0.0)
        high, low = split(jnp.concatenate([grid_ref[0], grid_ref[1]], axis=1))
        left = jnp.concatenate([high_ref[...], low_ref[...], high_ref[...]], axis=1)
        right = jnp.concatenate([high, high, low], axis=1)
        field_ref[...] = dot(left, right, ((1,), (1,)))
        for d in range(blocks):
            outs[d][...] = field_ref[pl.ds(pl.multiple_of((me ^ d) * rows, SUB), rows), :]

    return body


def quarter_swap(value):
    top = jnp.concatenate([value[:N, :N], value[N:, :N]], axis=1)
    bottom = jnp.concatenate([value[:N, N:], value[N:, N:]], axis=1)
    return jnp.concatenate([top, bottom], axis=0)


def strides(planes):
    gap = SUB if planes % SUB == 0 else 0
    return planes + gap, 2 * planes + gap


def plane_kernel(blocks, per_block, sticks, planes):
    rows = 2 * planes
    fold = LANES // rows
    reach = N * N // fold
    reach_bits = reach.bit_length() - 1
    span = N // fold
    slots = per_block * LANES
    plane_rows = min(planes, SUB)
    along_stride, back_stride = strides(planes)
    unroll = UNROLL

    def body(*refs):
        fields = refs[:blocks]
        smem_ref, cols_ref, v_ref, dv_ref, mh_ref, ml_ref, th_ref, tl_ref = refs[blocks : blocks + 8]
        outs = refs[blocks + 8 : 2 * blocks + 8]
        stick_ref, grid_ref, re_ref, im_ref, back_ref = refs[2 * blocks + 8 :]
        me = lax.axis_index("pencil")

        def right_apply(value, high_ref, low_ref):
            high, low = split(value)
            left = jnp.concatenate([high, low, high], axis=1)
            right = jnp.concatenate([high_ref[...], high_ref[...], low_ref[...]], axis=0)
            return dot(left, right, ((1,), (0,)))

        def left_apply(value, high_ref, low_ref):
            high, low = split(value)
            left = jnp.concatenate([high_ref[...], low_ref[...], high_ref[...]], axis=1)
            right = jnp.concatenate([high, high, low], axis=0)
            return dot(left, right, ((1,), (0,)))

        def each_stick(work):
            def block(q, c):
                def group(i, c2):
                    first = pl.multiple_of(q * slots + i * unroll, unroll)
                    at = q * sticks + i * unroll
                    for j in range(unroll):
                        work(first + j, smem_ref[at + j])
                    return c2

                return lax.fori_loop(0, sticks // unroll, group, c)

            lax.fori_loop(0, blocks, block, 0)

        grid_ref[...] = jnp.zeros(grid_ref.shape, jnp.float32)
        for d in range(blocks):
            base = pl.multiple_of((me ^ d) * slots, LANES)
            for k in range(per_block):
                w = min(LANES, sticks - k * LANES)
                part = fields[d][:, k * LANES : k * LANES + w]
                sub = cols_ref[pl.ds((me ^ d) * per_block + k, 1), :w] >> reach_bits
                part = jnp.concatenate([jnp.where(sub == u, part, 0.0) for u in range(fold)], axis=0)
                stick_ref[pl.ds(base + k * LANES, w), :] = part.T

        def scatter(stick, place):
            value = stick_ref[pl.ds(stick, 1), :]
            pltpu.store(grid_ref.at[pl.ds(place, 1), :], value, mask=value != 0.0)

        each_stick(scatter)

        step = 2 * N // planes

        def along(i, c):
            pieces = []
            for t in range(step // fold):
                at = pl.multiple_of((i * (step // fold) + t) * N, N)
                tile = grid_ref[pl.ds(at, N), :].T
                for u in range(fold):
                    lo = u * rows
                    pieces.append(jnp.concatenate([tile[lo : lo + planes], tile[lo + planes : lo + rows]], axis=1))
            value = right_apply(jnp.concatenate(pieces, axis=0), mh_ref, ml_ref)
            for x in range(step):
                at = ((x % fold) * span + i * (step // fold) + x // fold) * along_stride
                at = pl.multiple_of(at, SUB) if along_stride % SUB == 0 else at
                re_ref[pl.ds(at, planes), :] = value[x * planes : (x + 1) * planes, :N]
                im_ref[pl.ds(at, planes), :] = value[x * planes : (x + 1) * planes, N:]
            return c

        lax.fori_loop(0, N // step, along, 0)

        def pair(pp):
            tops, bottoms, weights = [], [], []
            for h in range(2):
                plane = pp * 2 + h
                pick = pl.ds(plane, N, stride=along_stride)
                tops.append(re_ref[pick, :])
                bottoms.append(im_ref[pick, :])
                at = pl.ds((plane // plane_rows) * (plane_rows * N) + plane % plane_rows, N, stride=plane_rows)
                weights.append(v_ref[at, :] + dv_ref[at, :])
            field = jnp.concatenate([jnp.concatenate(tops, axis=1), jnp.concatenate(bottoms, axis=1)], axis=0)
            space = left_apply(field, th_ref, tl_ref)
            weight = jnp.concatenate(weights, axis=1)
            space = space * jnp.concatenate([weight, weight], axis=0)
            back = left_apply(space, mh_ref, ml_ref)
            last = right_apply(quarter_swap(back), th_ref, tl_ref)
            for h in range(2):
                for part in range(2):
                    at = pl.ds(part * planes + pp * 2 + h, N, stride=back_stride)
                    back_ref[at, :] = last[h * N : (h + 1) * N, part * N : (part + 1) * N]

        def pairs(i, c):
            for j in range(2):
                pair(i * 2 + j)
            return c

        lax.fori_loop(0, planes // 4, pairs, 0)

        def turn(g, c):
            for j in range(4):
                i = g * 4 + j
                pieces = []
                for u in range(fold):
                    at = (u * span + i) * back_stride
                    pieces.append(back_ref[pl.ds(pl.multiple_of(at, SUB), rows), :])
                grid_ref[pl.ds(pl.multiple_of(i * N, N), N), :] = jnp.concatenate(pieces, axis=0).T
            return c

        lax.fori_loop(0, span // 4, turn, 0)

        def fetch(stick, place):
            stick_ref[pl.ds(stick, 1), :] = grid_ref[pl.ds(place, 1), :]

        each_stick(fetch)

        for d in range(blocks):
            for k in range(per_block):
                w = min(LANES, sticks - k * LANES)
                at = (me ^ d) * per_block + k
                tile = stick_ref[pl.ds(pl.multiple_of(at * LANES, LANES), LANES), :].T
                sub = cols_ref[pl.ds(at, 1), :] >> reach_bits
                value = tile[:rows]
                for u in range(1, fold):
                    value = jnp.where(sub == u, tile[u * rows : (u + 1) * rows], value)
                outs[d][:, k * LANES : k * LANES + w] = value[:, :w]

    return body


def down_kernel(blocks, rows, zpw):
    def body(*refs):
        fields = refs[:blocks]
        pw_ref, high_ref, low_ref, own_ref, other_ref, field_ref, grid_ref = refs[blocks:]
        me = lax.axis_index("pencil")
        first = lax.axis_index("tgroup") == 0
        for d in range(blocks):
            field_ref[pl.ds(pl.multiple_of((me ^ d) * rows, SUB), rows), :] = fields[d][...]
        high, low = split(field_ref[...])
        left = jnp.concatenate([high, low, high], axis=0)
        right = jnp.concatenate([high_ref[...], high_ref[...], low_ref[...]], axis=0)
        grid = dot(left, right, ((0,), (0,)))
        pairs = grid.shape[0] // 2
        half = pairs // 2
        even = pl.ds(0, pairs, stride=2)
        odd = pl.ds(1, pairs, stride=2)
        lane = lax.broadcasted_iota(jnp.int32, (pairs, LANES), 1)
        index = jnp.where(lane < zpw, pw_ref[even, :], pw_ref[odd, :])
        for part in range(2):
            grid_ref[part] = grid[:, part * N : (part + 1) * N]
            a = lane_gather(grid_ref[part, even, :], index)
            b = lane_gather(grid_ref[part, odd, :], index)
            picked = jnp.where(lane < zpw, a, b)
            own_ref[part] = jnp.where(first, picked[:half], picked[half:])
            other_ref[part] = jnp.where(first, picked[half:], picked[:half])

    return body


def call(body, outs, scratch, args, smem=(), room=16, flops=1 << 30):
    vmem = pl.BlockSpec(memory_space=pltpu.VMEM)
    scalar = pl.BlockSpec(memory_space=pltpu.SMEM)
    many = isinstance(outs, (list, tuple))
    return pl.pallas_call(
        body,
        out_shape=outs,
        in_specs=[scalar if i in smem else vmem for i in range(len(args))],
        out_specs=[vmem] * len(outs) if many else vmem,
        scratch_shapes=scratch,
        compiler_params=pltpu.CompilerParams(vmem_limit_bytes=room << 20),
        cost_estimate=pl.CostEstimate(flops=flops, bytes_accessed=1 << 20, transcendentals=0),
    )(*args)


def local(dpsi, stick_cols, pw_z, v_local, dv):
    blocks = lax.axis_size("pencil")
    bands = dpsi.shape[1]
    sticks, zpw = pw_z.shape
    planes = v_local.shape[0]
    rows = 2 * planes
    pairs = sticks // 2
    half = pairs // 2
    per_block = -(-sticks // LANES)
    f32 = jnp.float32
    first = lax.axis_index("tgroup") == 0

    matrix = transform_matrix()
    mh, ml = const_split(matrix)
    th, tl = const_split(matrix.T)
    order = np.arange(2 * N).reshape(2, blocks, planes).transpose(1, 0, 2).reshape(-1)
    uh, ul = const_split(matrix.T[order])
    dh, dl = const_split(matrix.T[order])

    swap = [(0, 1), (1, 0)]
    own = dpsi.reshape(2, bands, half, LANES).transpose(0, 2, 1, 3).reshape(2, half * bands, LANES)
    other = lax.ppermute(own, "tgroup", swap)

    lookup = jax.ShapeDtypeStruct((sticks, N), jnp.int32)
    inv, twice = call(stick_index_kernel(zpw), (lookup, lookup), [], (pw_z.T,))
    width = min(LANES, sticks)
    cols = stick_cols.reshape(blocks * per_block, width)
    if width < LANES:
        cols = jnp.pad(cols, ((0, 0), (0, LANES - width)), constant_values=-1)
    block = jax.ShapeDtypeStruct((rows, sticks), f32)
    fields = call(
        up_kernel(blocks, rows, zpw),
        [block] * blocks,
        [pltpu.VMEM((2, sticks, N), f32), pltpu.VMEM((2 * N, sticks), f32)],
        (own, other, inv, uh, ul),
    )

    def exchange(parts):
        got = [parts[0]]
        for d in range(1, blocks):
            got.append(lax.ppermute(parts[d], "pencil", [(i, i ^ d) for i in range(blocks)]))
        return got

    plane_rows = min(planes, SUB)

    def by_column(values):
        return (
            values.reshape(planes // plane_rows, plane_rows, N, N)
            .transpose(0, 2, 1, 3)
            .reshape(planes * N, N)
        )

    fold = LANES // rows
    along_stride, back_stride = strides(planes)
    applied = call(
        plane_kernel(blocks, per_block, sticks, planes),
        [block] * blocks,
        [
            pltpu.VMEM((blocks * per_block * LANES, LANES), f32),
            pltpu.VMEM((N // fold * N, LANES), f32),
            pltpu.VMEM((N * along_stride, N), f32),
            pltpu.VMEM((N * along_stride, N), f32),
            pltpu.VMEM((N * back_stride, N), f32),
        ],
        (*exchange(fields), stick_cols & (N * N // fold - 1), cols, by_column(v_local), by_column(dv), mh, ml, th, tl),
        smem=(blocks,),
        room=24,
        flops=1 << 33,
    )
    side = jax.ShapeDtypeStruct((2, half, LANES), f32)
    mine, theirs = call(
        down_kernel(blocks, rows, zpw),
        [side, side],
        [pltpu.VMEM((2 * N, sticks), f32), pltpu.VMEM((2, sticks, N), f32)],
        (*exchange(applied), twice, dh, dl),
    )
    back = lax.ppermute(theirs, "tgroup", swap)
    mine = mine.reshape(2, 1, half * LANES)
    back = back.reshape(2, 1, half * LANES)
    band = lax.broadcasted_iota(jnp.int32, (2, bands, half * LANES), 1)
    return jnp.where(band == lax.axis_index("tgroup"), mine, back)


def solution(mesh):
    in_specs = (
        P(None, "pool", ("pencil", "tgroup")),
        P(),
        P("pencil", None),
        P("pencil", None),
        P("pencil", None),
    )
    out_specs = P(None, "pool", ("pencil", "tgroup"))
    return jax.shard_map(local, mesh=mesh, in_specs=in_specs, out_specs=out_specs, check_vma=False)
```

```python
import math

import jax
import jax.numpy as jnp
import numpy as np
from jax import lax
from jax.experimental import pallas as pl
from jax.experimental.pallas import tpu as pltpu
from jax.sharding import PartitionSpec as P


N = 128
LANES = 128
SUB = 8
GROUP = 8


def transform_matrix():
    phase = np.outer(np.arange(N), np.arange(N)) % N
    angle = phase.astype(np.float64) * (2.0 * math.pi / N)
    re = np.cos(angle) / math.sqrt(N)
    im = np.sin(angle) / math.sqrt(N)
    return np.block([[re, im], [-im, re]])


def const_split(table):
    bf = jnp.bfloat16
    t32 = np.asarray(table, np.float32)
    high = t32.astype(bf)
    low = (t32 - high.astype(np.float32)).astype(bf)
    return jnp.asarray(high), jnp.asarray(low)


def split(value):
    high = value.astype(jnp.bfloat16)
    low = (value - high.astype(jnp.float32)).astype(jnp.bfloat16)
    return high, low


def dot(a, b, dims):
    return lax.dot_general(a, b, (dims, ((), ())), preferred_element_type=jnp.float32)


def lane_gather(values, index):
    return jnp.take_along_axis(values, index, axis=1, mode="promise_in_bounds")


def stick_index_kernel(zpw):
    def body(pw_ref, inv_ref, twice_ref):
        sticks = inv_ref.shape[0]
        for at in range(0, sticks, LANES):
            w = min(LANES, sticks - at)
            pw = pw_ref[:, at : at + w]
            spread = lax.broadcasted_iota(jnp.int32, (N, w), 0)
            acc = jnp.full((N, w), -1, jnp.int32)
            for k in range(zpw):
                acc = jnp.where(pw[k : k + 1, :] == spread, k, acc)
            inv_ref[at : at + w, :] = acc.T
            twice_ref[at : at + w, :] = jnp.concatenate([pw, pw], axis=0).T

    return body


def up_kernel(blocks, rows, zpw):
    def body(own_ref, other_ref, inv_ref, high_ref, low_ref, *rest):
        outs = rest[:blocks]
        grid_ref, field_ref = rest[blocks:]
        me = lax.axis_index("pencil")
        first = lax.axis_index("tgroup") == 0
        pairs = inv_ref.shape[0] // 2
        half = pairs // 2

        def mine(ref, part):
            low = ref[part, pl.ds(0, half, stride=2), :]
            high = ref[part, pl.ds(1, half, stride=2), :]
            return jnp.where(first, low, high)

        for part in range(2):
            own = mine(own_ref, part)
            other = mine(other_ref, part)
            coeff = jnp.concatenate([jnp.where(first, own, other), jnp.where(first, other, own)], axis=0)
            for parity in range(2):
                index = inv_ref[pl.ds(parity, pairs, stride=2), :]
                value = lane_gather(coeff, jnp.maximum(index, 0) + parity * zpw)
                grid_ref[part, pl.ds(parity, pairs, stride=2), :] = jnp.where(index >= 0, value, 0.0)
        high, low = split(jnp.concatenate([grid_ref[0], grid_ref[1]], axis=1))
        left = jnp.concatenate([high_ref[...], low_ref[...], high_ref[...]], axis=1)
        right = jnp.concatenate([high, high, low], axis=1)
        field_ref[...] = dot(left, right, ((1,), (1,)))
        for d in range(blocks):
            outs[d][...] = field_ref[pl.ds(pl.multiple_of((me ^ d) * rows, SUB), rows), :]

    return body


def quarter_swap(value):
    top = jnp.concatenate([value[:N, :N], value[N:, :N]], axis=1)
    bottom = jnp.concatenate([value[:N, N:], value[N:, N:]], axis=1)
    return jnp.concatenate([top, bottom], axis=0)


def strides(planes):
    return planes + 1, 2 * planes + 1


def plane_kernel(blocks, per_block, sticks, planes):
    rows = 2 * planes
    fold = LANES // rows
    reach = N * N // fold
    reach_bits = reach.bit_length() - 1
    span = N // fold
    slots = per_block * LANES
    plane_rows = min(planes, SUB)
    along_stride, back_stride = strides(planes)

    def body(*refs):
        fields = refs[:blocks]
        smem_ref, cols_ref, v_ref, dv_ref, mh_ref, ml_ref, th_ref, tl_ref = refs[blocks : blocks + 8]
        outs = refs[blocks + 8 : 2 * blocks + 8]
        stick_ref, grid_ref, re_ref, im_ref, back_ref = refs[2 * blocks + 8 :]
        me = lax.axis_index("pencil")

        def right_apply(value, high_ref, low_ref):
            high, low = split(value)
            left = jnp.concatenate([high, low, high], axis=1)
            right = jnp.concatenate([high_ref[...], high_ref[...], low_ref[...]], axis=0)
            return dot(left, right, ((1,), (0,)))

        def left_apply(value, high_ref, low_ref):
            high, low = split(value)
            left = jnp.concatenate([high_ref[...], low_ref[...], high_ref[...]], axis=1)
            right = jnp.concatenate([high, high, low], axis=0)
            return dot(left, right, ((1,), (0,)))

        def each_stick(work):
            for q in range(blocks):
                for j in range(sticks):
                    work(q * slots + j, smem_ref[q * sticks + j])

        grid_ref[...] = jnp.zeros(grid_ref.shape, jnp.float32)
        for d in range(blocks):
            base = pl.multiple_of((me ^ d) * slots, LANES)
            for k in range(per_block):
                w = min(LANES, sticks - k * LANES)
                part = fields[d][:, k * LANES : k * LANES + w]
                sub = cols_ref[pl.ds((me ^ d) * per_block + k, 1), :w] >> reach_bits
                part = jnp.concatenate([jnp.where(sub == u, part, 0.0) for u in range(fold)], axis=0)
                stick_ref[pl.ds(base + k * LANES, w), :] = part.T

        def scatter(stick, place):
            value = stick_ref[pl.ds(stick, 1), :]
            pltpu.store(grid_ref.at[pl.ds(place, 1), :], value, mask=value != 0.0)

        each_stick(scatter)

        step = 2 * N // planes

        def along_load(i):
            pieces = []
            for t in range(step // fold):
                at = pl.multiple_of((i * (step // fold) + t) * N, N)
                tile = grid_ref[pl.ds(at, N), :].T
                for u in range(fold):
                    lo = u * rows
                    pieces.append(jnp.concatenate([tile[lo : lo + planes], tile[lo + planes : lo + rows]], axis=1))
            return jnp.concatenate(pieces, axis=0)

        def along_store(i, value):
            for x in range(step):
                at = ((x % fold) * span + i * (step // fold) + x // fold) * along_stride
                re_ref[pl.ds(at, planes), :] = value[x * planes : (x + 1) * planes, :N]
                im_ref[pl.ds(at, planes), :] = value[x * planes : (x + 1) * planes, N:]

        many = min(GROUP, N // step)

        def along(g, c):
            own = [g * many + j for j in range(many)]
            values = [along_load(i) for i in own]
            values = [right_apply(value, mh_ref, ml_ref) for value in values]
            for i, value in zip(own, values):
                along_store(i, value)
            return c

        lax.fori_loop(0, N // step // many, along, 0)

        def load_pair(pp):
            tops, bottoms = [], []
            for h in range(2):
                pick = pl.ds(pp * 2 + h, N, stride=along_stride)
                tops.append(re_ref[pick, :])
                bottoms.append(im_ref[pick, :])
            return jnp.concatenate([jnp.concatenate(tops, axis=1), jnp.concatenate(bottoms, axis=1)], axis=0)

        def weigh(pp, space):
            weights = []
            for h in range(2):
                plane = pp * 2 + h
                at = pl.ds((plane // plane_rows) * (plane_rows * N) + plane % plane_rows, N, stride=plane_rows)
                weights.append(v_ref[at, :] + dv_ref[at, :])
            weight = jnp.concatenate(weights, axis=1)
            return space * jnp.concatenate([weight, weight], axis=0)

        def store_pair(pp, last):
            for h in range(2):
                for part in range(2):
                    at = pl.ds(part * planes + pp * 2 + h, N, stride=back_stride)
                    back_ref[at, :] = last[h * N : (h + 1) * N, part * N : (part + 1) * N]

        group = min(GROUP, planes // 2)

        def pairs(i, c):
            own = [i * group + j for j in range(group)]
            values = [left_apply(load_pair(pp), th_ref, tl_ref) for pp in own]
            values = [weigh(pp, value) for pp, value in zip(own, values)]
            values = [left_apply(value, mh_ref, ml_ref) for value in values]
            values = [right_apply(quarter_swap(value), th_ref, tl_ref) for value in values]
            for pp, value in zip(own, values):
                store_pair(pp, value)
            return c

        lax.fori_loop(0, planes // 2 // group, pairs, 0)

        def turn(g, c):
            for j in range(4):
                i = g * 4 + j
                pieces = []
                for u in range(fold):
                    at = (u * span + i) * back_stride
                    pieces.append(back_ref[pl.ds(at, rows), :])
                grid_ref[pl.ds(pl.multiple_of(i * N, N), N), :] = jnp.concatenate(pieces, axis=0).T
            return c

        lax.fori_loop(0, span // 4, turn, 0)

        def fetch(stick, place):
            stick_ref[pl.ds(stick, 1), :] = grid_ref[pl.ds(place, 1), :]

        each_stick(fetch)

        for d in range(blocks):
            for k in range(per_block):
                w = min(LANES, sticks - k * LANES)
                at = (me ^ d) * per_block + k
                tile = stick_ref[pl.ds(pl.multiple_of(at * LANES, LANES), LANES), :].T
                sub = cols_ref[pl.ds(at, 1), :] >> reach_bits
                value = tile[:rows]
                for u in range(1, fold):
                    value = jnp.where(sub == u, tile[u * rows : (u + 1) * rows], value)
                outs[d][:, k * LANES : k * LANES + w] = value[:, :w]

    return body


def down_kernel(blocks, rows, zpw):
    def body(*refs):
        fields = refs[:blocks]
        pw_ref, high_ref, low_ref, own_ref, other_ref, field_ref, grid_ref = refs[blocks:]
        me = lax.axis_index("pencil")
        first = lax.axis_index("tgroup") == 0
        for d in range(blocks):
            field_ref[pl.ds(pl.multiple_of((me ^ d) * rows, SUB), rows), :] = fields[d][...]
        high, low = split(field_ref[...])
        left = jnp.concatenate([high, low, high], axis=0)
        right = jnp.concatenate([high_ref[...], high_ref[...], low_ref[...]], axis=0)
        grid = dot(left, right, ((0,), (0,)))
        pairs = grid.shape[0] // 2
        half = pairs // 2
        even = pl.ds(0, pairs, stride=2)
        odd = pl.ds(1, pairs, stride=2)
        lane = lax.broadcasted_iota(jnp.int32, (pairs, LANES), 1)
        index = jnp.where(lane < zpw, pw_ref[even, :], pw_ref[odd, :])
        for part in range(2):
            grid_ref[part] = grid[:, part * N : (part + 1) * N]
            a = lane_gather(grid_ref[part, even, :], index)
            b = lane_gather(grid_ref[part, odd, :], index)
            picked = jnp.where(lane < zpw, a, b)
            own_ref[part] = jnp.where(first, picked[:half], picked[half:])
            other_ref[part] = jnp.where(first, picked[half:], picked[:half])

    return body


def call(body, outs, scratch, args, smem=(), room=16, flops=1 << 30):
    vmem = pl.BlockSpec(memory_space=pltpu.VMEM)
    scalar = pl.BlockSpec(memory_space=pltpu.SMEM)
    many = isinstance(outs, (list, tuple))
    return pl.pallas_call(
        body,
        out_shape=outs,
        in_specs=[scalar if i in smem else vmem for i in range(len(args))],
        out_specs=[vmem] * len(outs) if many else vmem,
        scratch_shapes=scratch,
        compiler_params=pltpu.CompilerParams(vmem_limit_bytes=room << 20),
        cost_estimate=pl.CostEstimate(flops=flops, bytes_accessed=1 << 20, transcendentals=0),
    )(*args)


def local(dpsi, stick_cols, pw_z, v_local, dv):
    blocks = lax.axis_size("pencil")
    bands = dpsi.shape[1]
    sticks, zpw = pw_z.shape
    planes = v_local.shape[0]
    rows = 2 * planes
    pairs = sticks // 2
    half = pairs // 2
    per_block = -(-sticks // LANES)
    f32 = jnp.float32

    matrix = transform_matrix()
    mh, ml = const_split(matrix)
    th, tl = const_split(matrix.T)
    order = np.arange(2 * N).reshape(2, blocks, planes).transpose(1, 0, 2).reshape(-1)
    uh, ul = const_split(matrix.T[order])
    dh, dl = const_split(matrix.T[order])

    swap = [(0, 1), (1, 0)]
    own = dpsi.reshape(2, bands, half, LANES).transpose(0, 2, 1, 3).reshape(2, half * bands, LANES)
    other = lax.ppermute(own, "tgroup", swap)

    lookup = jax.ShapeDtypeStruct((sticks, N), jnp.int32)
    inv, twice = call(stick_index_kernel(zpw), (lookup, lookup), [], (pw_z.T,))
    width = min(LANES, sticks)
    cols = stick_cols.reshape(blocks * per_block, width)
    if width < LANES:
        cols = jnp.pad(cols, ((0, 0), (0, LANES - width)), constant_values=-1)
    block = jax.ShapeDtypeStruct((rows, sticks), f32)
    fields = call(
        up_kernel(blocks, rows, zpw),
        [block] * blocks,
        [pltpu.VMEM((2, sticks, N), f32), pltpu.VMEM((2 * N, sticks), f32)],
        (own, other, inv, uh, ul),
    )

    def exchange(parts):
        got = [parts[0]]
        for d in range(1, blocks):
            got.append(lax.ppermute(parts[d], "pencil", [(i, i ^ d) for i in range(blocks)]))
        return got

    plane_rows = min(planes, SUB)

    def by_column(values):
        return (
            values.reshape(planes // plane_rows, plane_rows, N, N)
            .transpose(0, 2, 1, 3)
            .reshape(planes * N, N)
        )

    fold = LANES // rows
    along_stride, back_stride = strides(planes)
    applied = call(
        plane_kernel(blocks, per_block, sticks, planes),
        [block] * blocks,
        [
            pltpu.VMEM((blocks * per_block * LANES, LANES), f32),
            pltpu.VMEM((N // fold * N, LANES), f32),
            pltpu.VMEM((N * along_stride, N), f32),
            pltpu.VMEM((N * along_stride, N), f32),
            pltpu.VMEM((N * back_stride, N), f32),
        ],
        (*exchange(fields), stick_cols & (N * N // fold - 1), cols, by_column(v_local), by_column(dv), mh, ml, th, tl),
        smem=(blocks,),
        room=24,
        flops=1 << 33,
    )
    side = jax.ShapeDtypeStruct((2, half, LANES), f32)
    mine, theirs = call(
        down_kernel(blocks, rows, zpw),
        [side, side],
        [pltpu.VMEM((2 * N, sticks), f32), pltpu.VMEM((2, sticks, N), f32)],
        (*exchange(applied), twice, dh, dl),
    )
    back = lax.ppermute(theirs, "tgroup", swap)
    mine = mine.reshape(2, 1, half * LANES)
    back = back.reshape(2, 1, half * LANES)
    band = lax.broadcasted_iota(jnp.int32, (2, bands, half * LANES), 1)
    return jnp.where(band == lax.axis_index("tgroup"), mine, back)


def solution(mesh):
    in_specs = (
        P(None, "pool", ("pencil", "tgroup")),
        P(),
        P("pencil", None),
        P("pencil", None),
        P("pencil", None),
    )
    out_specs = P(None, "pool", ("pencil", "tgroup"))

    return jax.shard_map(local, mesh=mesh, in_specs=in_specs, out_specs=out_specs, check_vma=False)
```

```python
import math

import jax
import jax.numpy as jnp
import numpy as np
from jax import lax
from jax.experimental import pallas as pl
from jax.experimental.pallas import tpu as pltpu
from jax.sharding import PartitionSpec as P


N = 128
LANES = 128
SUB = 8
GROUP = 8
EXTRA = 1
ORDER = (6, 4, 7, 5, 2, 3, 1)


def transform_matrix():
    phase = np.outer(np.arange(N), np.arange(N)) % N
    angle = phase.astype(np.float64) * (2.0 * math.pi / N)
    re = np.cos(angle) / math.sqrt(N)
    im = np.sin(angle) / math.sqrt(N)
    return np.block([[re, im], [-im, re]])


def const_split(table):
    bf = jnp.bfloat16
    t32 = np.asarray(table, np.float32)
    high = t32.astype(bf)
    low = (t32 - high.astype(np.float32)).astype(bf)
    return jnp.asarray(high), jnp.asarray(low)


def split(value):
    high = value.astype(jnp.bfloat16)
    low = (value - high.astype(jnp.float32)).astype(jnp.bfloat16)
    return high, low


def dot(a, b, dims):
    return lax.dot_general(a, b, (dims, ((), ())), preferred_element_type=jnp.float32)


def lane_gather(values, index):
    return jnp.take_along_axis(values, index, axis=1, mode="promise_in_bounds")


def stick_index_kernel(zpw):
    def body(pw_ref, inv_ref, twice_ref):
        sticks = inv_ref.shape[0]
        for at in range(0, sticks, LANES):
            w = min(LANES, sticks - at)
            pw = pw_ref[:, at : at + w]
            small = pw.astype(jnp.float32).astype(jnp.bfloat16)
            spread = lax.broadcasted_iota(jnp.int32, (N, w), 0).astype(jnp.float32).astype(jnp.bfloat16)
            acc = jnp.full((N, w), -1.0, jnp.bfloat16)
            for k in range(zpw):
                acc = jnp.where(small[k : k + 1, :] == spread, jnp.bfloat16(k), acc)
            inv_ref[at : at + w, :] = acc.astype(jnp.float32).T.astype(jnp.int32)
            twice_ref[at : at + w, :] = jnp.concatenate([pw, pw], axis=0).T

    return body


def up_kernel(blocks, rows, zpw, reach):
    def body(own_ref, other_ref, inv_ref, high_ref, low_ref, all_ref, *rest):
        outs = rest[:blocks]
        cols_ref, place_ref, grid_ref, field_ref = rest[blocks:]
        me = lax.axis_index("pencil")
        per_block = cols_ref.shape[0] // blocks
        for d in range(blocks):
            for k in range(per_block):
                row = all_ref[pl.ds((me ^ d) * per_block + k, 1), :]
                at = d * per_block + k
                cols_ref[at : at + 1, :] = row
                place_ref[at : at + 1, :] = row & (reach - 1)
        first = lax.axis_index("tgroup") == 0
        pairs = inv_ref.shape[0] // 2
        half = pairs // 2

        def mine(ref, part):
            low = ref[part, pl.ds(0, half, stride=2), :]
            high = ref[part, pl.ds(1, half, stride=2), :]
            return jnp.where(first, low, high)

        for part in range(2):
            own = mine(own_ref, part)
            other = mine(other_ref, part)
            coeff = jnp.concatenate([jnp.where(first, own, other), jnp.where(first, other, own)], axis=0)
            for parity in range(2):
                index = inv_ref[pl.ds(parity, pairs, stride=2), :]
                value = lane_gather(coeff, jnp.maximum(index, 0) + parity * zpw)
                grid_ref[part, pl.ds(parity, pairs, stride=2), :] = jnp.where(index >= 0, value, 0.0)
        high, low = split(jnp.concatenate([grid_ref[0], grid_ref[1]], axis=1))
        left = jnp.concatenate([high_ref[...], low_ref[...], high_ref[...]], axis=1)
        right = jnp.concatenate([high, high, low], axis=1)
        field_ref[...] = dot(left, right, ((1,), (1,)))
        for d in range(blocks):
            outs[d][...] = field_ref[pl.ds(pl.multiple_of((me ^ d) * rows, SUB), rows), :]

    return body


def quarter_swap(value):
    top = jnp.concatenate([value[:N, :N], value[N:, :N]], axis=1)
    bottom = jnp.concatenate([value[:N, N:], value[N:, N:]], axis=1)
    return jnp.concatenate([top, bottom], axis=0)


def strides(planes):
    return planes + 1, 2 * planes + 1


def place_sticks(ids, fields, smem_ref, cols_ref, stick_ref, grid_ref):
    rows, sticks = fields[0].shape
    fold = LANES // rows
    reach_bits = (N * N // fold).bit_length() - 1
    per_block = -(-sticks // LANES)
    for n, d in enumerate(ids):
        for k in range(per_block):
            w = min(LANES, sticks - k * LANES)
            part = fields[n][:, k * LANES : k * LANES + w]
            sub = cols_ref[d * per_block + k : d * per_block + k + 1, :w] >> reach_bits
            part = jnp.concatenate([jnp.where(sub == u, part, 0.0) for u in range(fold)], axis=0)
            at = (n * per_block + k) * LANES
            stick_ref[at : at + w, :] = part.T
    for n, d in enumerate(ids):
        for j in range(sticks):
            at = n * per_block * LANES + j
            value = stick_ref[at : at + 1, :]
            pltpu.store(grid_ref.at[pl.ds(smem_ref[d * sticks + j], 1), :], value, mask=value != 0.0)


def take_sticks(ids, outs, smem_ref, cols_ref, stick_ref, grid_ref):
    rows, sticks = outs[0].shape
    fold = LANES // rows
    reach_bits = (N * N // fold).bit_length() - 1
    per_block = -(-sticks // LANES)
    for n, d in enumerate(ids):
        for j in range(sticks):
            at = n * per_block * LANES + j
            stick_ref[at : at + 1, :] = grid_ref[pl.ds(smem_ref[d * sticks + j], 1), :]
    for n, d in enumerate(ids):
        for k in range(per_block):
            w = min(LANES, sticks - k * LANES)
            at = (n * per_block + k) * LANES
            tile = stick_ref[at : at + LANES, :].T
            sub = cols_ref[d * per_block + k : d * per_block + k + 1, :] >> reach_bits
            value = tile[:rows]
            for u in range(1, fold):
                value = jnp.where(sub == u, tile[u * rows : (u + 1) * rows], value)
            outs[n][:, k * LANES : k * LANES + w] = value[:, :w]


def early_kernel(ids):
    def body(*refs):
        fields = refs[: len(ids)]
        smem_ref, cols_ref, grid_ref, stick_ref = refs[len(ids) :]
        grid_ref[...] = jnp.zeros(grid_ref.shape, jnp.float32)
        place_sticks(ids, fields, smem_ref, cols_ref, stick_ref, grid_ref)

    return body


def late_kernel(ids):
    def body(grid_ref, smem_ref, cols_ref, *rest):
        take_sticks(ids, rest[:-1], smem_ref, cols_ref, rest[-1], grid_ref)

    return body


def plane_kernel(ids_in, ids_out, planes):
    rows = 2 * planes
    fold = LANES // rows
    span = N // fold
    plane_rows = min(planes, SUB)
    along_stride, back_stride = strides(planes)
    count_in, count_out = len(ids_in), len(ids_out)

    def body(*refs):
        fields = refs[:count_in]
        _, smem_ref, cols_ref, v_ref, dv_ref, mh_ref, ml_ref, th_ref, tl_ref = refs[count_in : count_in + 9]
        grid_ref = refs[count_in + 9]
        outs = refs[count_in + 10 : count_in + 10 + count_out]
        stick_ref, re_ref, im_ref, back_ref = refs[count_in + 10 + count_out :]

        def right_apply(value, high_ref, low_ref):
            high, low = split(value)
            left = jnp.concatenate([high, low, high], axis=1)
            right = jnp.concatenate([high_ref[...], high_ref[...], low_ref[...]], axis=0)
            return dot(left, right, ((1,), (0,)))

        def left_apply(value, high_ref, low_ref):
            high, low = split(value)
            left = jnp.concatenate([high_ref[...], low_ref[...], high_ref[...]], axis=1)
            right = jnp.concatenate([high, high, low], axis=0)
            return dot(left, right, ((1,), (0,)))

        place_sticks(ids_in, fields, smem_ref, cols_ref, stick_ref, grid_ref)

        step = 2 * N // planes

        def along_load(i):
            pieces = []
            for t in range(step // fold):
                at = pl.multiple_of((i * (step // fold) + t) * N, N)
                tile = grid_ref[pl.ds(at, N), :].T
                for u in range(fold):
                    lo = u * rows
                    pieces.append(jnp.concatenate([tile[lo : lo + planes], tile[lo + planes : lo + rows]], axis=1))
            return jnp.concatenate(pieces, axis=0)

        def along_store(i, value):
            for x in range(step):
                at = ((x % fold) * span + i * (step // fold) + x // fold) * along_stride
                re_ref[pl.ds(at, planes), :] = value[x * planes : (x + 1) * planes, :N]
                im_ref[pl.ds(at, planes), :] = value[x * planes : (x + 1) * planes, N:]

        many = min(GROUP, N // step)

        def along(g, c):
            own = [g * many + j for j in range(many)]
            values = [along_load(i) for i in own]
            values = [right_apply(value, mh_ref, ml_ref) for value in values]
            for i, value in zip(own, values):
                along_store(i, value)
            return c

        lax.fori_loop(0, N // step // many, along, 0)

        def load_pair(pp):
            tops, bottoms = [], []
            for h in range(2):
                pick = pl.ds(pp * 2 + h, N, stride=along_stride)
                tops.append(re_ref[pick, :])
                bottoms.append(im_ref[pick, :])
            return jnp.concatenate([jnp.concatenate(tops, axis=1), jnp.concatenate(bottoms, axis=1)], axis=0)

        def weigh(pp, space):
            weights = []
            for h in range(2):
                plane = pp * 2 + h
                at = pl.ds((plane // plane_rows) * (plane_rows * N) + plane % plane_rows, N, stride=plane_rows)
                weights.append(v_ref[at, :] + dv_ref[at, :])
            weight = jnp.concatenate(weights, axis=1)
            return space * jnp.concatenate([weight, weight], axis=0)

        def store_pair(pp, last):
            for h in range(2):
                for part in range(2):
                    at = pl.ds(part * planes + pp * 2 + h, N, stride=back_stride)
                    back_ref[at, :] = last[h * N : (h + 1) * N, part * N : (part + 1) * N]

        group = min(GROUP, planes // 2)

        def pairs(i, c):
            own = [i * group + j for j in range(group)]
            values = [left_apply(load_pair(pp), th_ref, tl_ref) for pp in own]
            values = [weigh(pp, value) for pp, value in zip(own, values)]
            values = [left_apply(value, mh_ref, ml_ref) for value in values]
            values = [right_apply(quarter_swap(value), th_ref, tl_ref) for value in values]
            for pp, value in zip(own, values):
                store_pair(pp, value)
            return c

        lax.fori_loop(0, planes // 2 // group, pairs, 0)

        def turn(g, c):
            for j in range(4):
                i = g * 4 + j
                pieces = []
                for u in range(fold):
                    at = (u * span + i) * back_stride
                    pieces.append(back_ref[pl.ds(at, rows), :])
                grid_ref[pl.ds(pl.multiple_of(i * N, N), N), :] = jnp.concatenate(pieces, axis=0).T
            return c

        lax.fori_loop(0, span // 4, turn, 0)

        take_sticks(ids_out, outs, smem_ref, cols_ref, stick_ref, grid_ref)

    return body


def down_kernel(blocks, rows, zpw):
    def body(*refs):
        fields = refs[:blocks]
        pw_ref, high_ref, low_ref, own_ref, other_ref, field_ref, grid_ref = refs[blocks:]
        me = lax.axis_index("pencil")
        first = lax.axis_index("tgroup") == 0
        for d in range(blocks):
            field_ref[pl.ds(pl.multiple_of((me ^ d) * rows, SUB), rows), :] = fields[d][...]
        high, low = split(field_ref[...])
        left = jnp.concatenate([high, low, high], axis=0)
        right = jnp.concatenate([high_ref[...], high_ref[...], low_ref[...]], axis=0)
        grid = dot(left, right, ((0,), (0,)))
        pairs = grid.shape[0] // 2
        half = pairs // 2
        even = pl.ds(0, pairs, stride=2)
        odd = pl.ds(1, pairs, stride=2)
        lane = lax.broadcasted_iota(jnp.int32, (pairs, LANES), 1)
        index = jnp.where(lane < zpw, pw_ref[even, :], pw_ref[odd, :])
        for part in range(2):
            grid_ref[part] = grid[:, part * N : (part + 1) * N]
            a = lane_gather(grid_ref[part, even, :], index)
            b = lane_gather(grid_ref[part, odd, :], index)
            picked = jnp.where(lane < zpw, a, b)
            own_ref[part] = jnp.where(first, picked[:half], picked[half:])
            other_ref[part] = jnp.where(first, picked[half:], picked[:half])

    return body


def call(body, outs, scratch, args, smem=(), room=16, flops=1 << 30, alias=None):
    vmem = pl.BlockSpec(memory_space=pltpu.VMEM)
    scalar = pl.BlockSpec(memory_space=pltpu.SMEM)
    many = isinstance(outs, (list, tuple))
    return pl.pallas_call(
        body,
        out_shape=outs,
        in_specs=[scalar if i in smem else vmem for i in range(len(args))],
        out_specs=[vmem] * len(outs) if many else vmem,
        scratch_shapes=scratch,
        input_output_aliases=alias or {},
        compiler_params=pltpu.CompilerParams(vmem_limit_bytes=room << 20),
        cost_estimate=pl.CostEstimate(flops=flops, bytes_accessed=1 << 20, transcendentals=0),
    )(*args)


def local(dpsi, stick_cols, pw_z, v_local, dv):
    blocks = lax.axis_size("pencil")
    bands = dpsi.shape[1]
    sticks, zpw = pw_z.shape
    planes = v_local.shape[0]
    rows = 2 * planes
    pairs = sticks // 2
    half = pairs // 2
    per_block = -(-sticks // LANES)
    f32 = jnp.float32

    matrix = transform_matrix()
    mh, ml = const_split(matrix)
    th, tl = const_split(matrix.T)
    order = np.arange(2 * N).reshape(2, blocks, planes).transpose(1, 0, 2).reshape(-1)
    uh, ul = const_split(matrix.T[order])
    dh, dl = const_split(matrix.T[order])

    swap = [(0, 1), (1, 0)]
    own = dpsi.reshape(2, bands, half, LANES).transpose(0, 2, 1, 3).reshape(2, half * bands, LANES)
    other = lax.ppermute(own, "tgroup", swap)

    width = min(LANES, sticks)
    columns = stick_cols.reshape(blocks * per_block, width)
    if width < LANES:
        columns = jnp.pad(columns, ((0, 0), (0, LANES - width)))
    lookup = jax.ShapeDtypeStruct((sticks, N), jnp.int32)
    inv, twice = call(stick_index_kernel(zpw), (lookup, lookup), [], (pw_z.T,))

    block = jax.ShapeDtypeStruct((rows, sticks), f32)
    near = jax.ShapeDtypeStruct(columns.shape, jnp.int32)
    *fields, cols, places = call(
        up_kernel(blocks, rows, zpw, N * N // (LANES // rows)),
        [block] * blocks + [near, near],
        [pltpu.VMEM((2, sticks, N), f32), pltpu.VMEM((2 * N, sticks), f32)],
        (own, other, inv, uh, ul, columns),
    )
    places = places[:, :width].reshape(-1)

    order = issue_order(blocks)
    early = [0] + order[: blocks // 2 - 1] + order[blocks // 2 : blocks // 2 + EXTRA]
    rest = [d for d in order if d not in early]
    ahead = order
    behind = [0]

    def send(part, d):
        if d == 0:
            return part
        return lax.ppermute(part, "pencil", [(i, i ^ d) for i in range(blocks)])

    plane_rows = min(planes, SUB)

    def by_column(values):
        return (
            values.reshape(planes // plane_rows, plane_rows, N, N)
            .transpose(0, 2, 1, 3)
            .reshape(planes * N, N)
        )

    fold = LANES // rows
    along_stride, back_stride = strides(planes)
    reach = jax.ShapeDtypeStruct((N // fold * N, LANES), f32)

    def room_for(ids):
        return pltpu.VMEM((len(ids) * per_block * LANES, LANES), f32)

    got = {d: send(fields[d], d) for d in range(blocks)}
    grid = call(
        early_kernel(early),
        reach,
        [room_for(early)],
        (*[got[d] for d in early], places, cols),
        smem=(len(early),),
    )
    count = len(rest)
    grid, *first_out = call(
        plane_kernel(rest, ahead, planes),
        [reach] + [block] * len(ahead),
        [
            room_for(max(rest, ahead, key=len)),
            pltpu.VMEM((N * along_stride, N), f32),
            pltpu.VMEM((N * along_stride, N), f32),
            pltpu.VMEM((N * back_stride, N), f32),
        ],
        (*[got[d] for d in rest], grid, places, cols, by_column(v_local), by_column(dv), mh, ml, th, tl),
        smem=(count + 1,),
        room=24,
        flops=1 << 33,
        alias={count: 0},
    )
    last_out = call(late_kernel(behind), [block] * len(behind), [room_for(behind)], (grid, places, cols), smem=(1,))
    applied = dict(zip(ahead + behind, list(first_out) + list(last_out)))
    back = {d: send(applied[d], d) for d in range(blocks)}
    side = jax.ShapeDtypeStruct((2, half, LANES), f32)
    mine, theirs = call(
        down_kernel(blocks, rows, zpw),
        [side, side],
        [pltpu.VMEM((2 * N, sticks), f32), pltpu.VMEM((2, sticks, N), f32)],
        (*[back[d] for d in range(blocks)], twice, dh, dl),
    )
    theirs = lax.ppermute(theirs, "tgroup", swap)
    mine = mine.reshape(2, 1, half * LANES)
    back = theirs.reshape(2, 1, half * LANES)
    band = lax.broadcasted_iota(jnp.int32, (2, bands, half * LANES), 1)
    return jnp.where(band == lax.axis_index("tgroup"), mine, back)


def issue_order(count):
    return list(ORDER) if len(ORDER) == count - 1 else list(range(count - 1, 0, -1))


def solution(mesh):
    in_specs = (
        P(None, "pool", ("pencil", "tgroup")),
        P(),
        P("pencil", None),
        P("pencil", None),
        P("pencil", None),
    )
    out_specs = P(None, "pool", ("pencil", "tgroup"))

    return jax.shard_map(local, mesh=mesh, in_specs=in_specs, out_specs=out_specs, check_vma=False)
```
